32 devices in a mesh: tok: 8 (over y, x, core), exp: 4 (over z).
Axes of the slice: x: 2, y: 2, z: 4, core: 2. Of those that a mesh axis runs over, the one named last changes fastest.
Arguments:
- expert_rows: bfloat16 [4, 2048, 4096], P('exp', 'tok'), may hold values from -480 to 480
- router_input: bfloat16 [2048, 4096], P(('tok', 'exp')), may hold values from -6 to 6
- router_weight: float32 [4096, 4], replicated, may hold values from -0.09375 to 0.09375
- assign: int32 [2048, 2], P(('tok', 'exp')), may hold values from 0 to 3, all different within a row
- targets: int32 [2048], P(('tok', 'exp')), may hold values from 0 to 15999
- head: bfloat16 [4096, 16000], P('tok', 'exp'), may hold values from -0.35 to 0.35
Outputs:
- token_loss: float32 [2048], P(('tok', 'exp'))
- router_grad: float32 [4096, 4], replicated
- mean_loss: float32 [], replicated
The draws below stay inside these ranges and needn't reach their ends.
All inputs are finite; a program needn't handle non-finite values.
Results may differ from the reference program's by a relative error of at most 0.007.
Values may be sent and summed in bfloat16 or wider, within the bound.
A program may use at most 128 MiB of HBM per device.

```python
import math
import jax
import jax.numpy as jnp
import numpy as np
from jax import lax

DMODEL = 4096
EXPERTS = 4
VOCAB = 16000
TOKENS = 2048
N_EXP = 4


def head_table(key):
    base_key = jax.random.fold_in(key, 17)
    table = 0.08 * jax.random.truncated_normal(base_key, -4.0, 4.0, (DMODEL, VOCAB), jnp.float32)
    return table


def draw_head(key, part):
    return head_table(key).astype(jnp.bfloat16)


def drawn_rows(key, table):
    first_col = jax.random.randint(jax.random.fold_in(key, 37), (8,), 0, VOCAB)
    second_col = (first_col + jax.random.randint(jax.random.fold_in(key, 41), (8,), 1, VOCAB)) % VOCAB
    levels = jnp.array([110.0, 170.0, 240.0, 110.0, 170.0, 240.0, 170.0, 240.0], jnp.float32)
    near_cols = table[:, first_col].T
    far_cols = table[:, second_col].T
    near_norm = jnp.sum(near_cols * near_cols, axis=1)
    far_norm = jnp.sum(far_cols * far_cols, axis=1)
    cross = jnp.sum(near_cols * far_cols, axis=1)
    determinant = near_norm * far_norm - cross * cross
    lower = levels - 2.0
    near_coef = (levels * far_norm - lower * cross) / determinant
    far_coef = (lower * near_norm - levels * cross) / determinant
    aligned = near_coef[:, None] * near_cols + far_coef[:, None] * far_cols
    return jnp.clip(aligned, -480.0, 480.0)


def draw_expert_rows(key, part):
    base_key = jax.random.fold_in(key, 29)
    position = jnp.arange(TOKENS, dtype=jnp.float32) / max(TOKENS - 1, 1)
    values = jax.random.truncated_normal(base_key, -5.0, 5.0, (EXPERTS, TOKENS, DMODEL), jnp.float32)
    rising = jnp.exp(jnp.log(0.3) + position * (jnp.log(1.5) - jnp.log(0.3)))
    values = values * rising[None, :, None]
    table = head_table(key)
    chosen = jax.random.permutation(jax.random.fold_in(key, 31), TOKENS)[:8]
    aligned = drawn_rows(key, table)
    values = values.at[:, chosen, :].set(jnp.broadcast_to(aligned[None], (EXPERTS, 8, DMODEL)))
    return values.astype(jnp.bfloat16)


def set_ends(result, stream_key, least, largest):
    index_at = [jax.random.randint(jax.random.fold_in(stream_key, axis), (), 0, length) for axis, length in enumerate(result.shape)]
    widest = result.shape.index(max(result.shape))
    beside = index_at[:widest] + [(index_at[widest] + 1) % result.shape[widest]] + index_at[widest + 1:]
    return result.at[tuple(index_at)].set(least).at[tuple(beside)].set(largest)


def steps_of(rng, extent, pieces, low, largest):
    factor_of, own = 1.0, jax.random.fold_in(rng, 6)
    for dim, shards_of in pieces:
        heights = jnp.exp(jax.random.uniform(jax.random.fold_in(own, dim), (shards_of,), jnp.float32, low / len(pieces), largest / len(pieces)))
        factor_of = factor_of * jnp.repeat(heights, extent[dim] // shards_of).reshape([-1 if axis == dim else 1 for axis in range(len(extent))])
    return factor_of


def rank_table(amount, skew):
    loads = [(1 << 20) // math.isqrt(standing ** skew) + 1 for standing in range(1, amount + 1)]
    width = 1 + sum(loads) // (1 << 30)
    return np.cumsum(np.array([max(1, weight // width) for weight in loads]))


def ranked_ids(key, dims, number_of, skew):
    listing = rank_table(number_of, skew)
    pick = jax.random.randint(jax.random.fold_in(key, 1), dims, 0, int(listing[number_of - 1]))
    rank = jnp.searchsorted(jnp.asarray(listing, jnp.int32), pick, side="right")
    return jax.random.permutation(jax.random.fold_in(key, 2), number_of)[rank].astype(jnp.int32)


def picks_of(rng, rows, number_of, top, lift):
    ranking = jax.random.permutation(jax.random.fold_in(rng, 1), number_of)
    favour = ranking
    for power in range(3):
        favour = favour * favour // number_of
    favour = favour * lift // number_of
    lots = jax.random.randint(jax.random.fold_in(rng, 2), (rows, number_of), 0, 4096) + favour
    sure = jax.random.permutation(jax.random.fold_in(rng, 3), rows)[jnp.arange(number_of) % rows]
    lots = jnp.where(jnp.arange(rows)[:, None] == sure[None, :], 1 << 14, lots)
    merit = lots * number_of + jnp.arange(number_of)
    return lax.top_k(merit.astype(jnp.int32), top)[1].astype(jnp.int32)


def centred(rng, shape, deviation, reach, cuts=(), kind=jnp.bfloat16):
    entries = jax.random.normal(rng, shape, jnp.float32) * deviation
    if len(cuts) > 0:
        entries = steps_of(rng, shape, cuts, -0.22, 0.18) * entries
    return jnp.clip(entries, min=-reach, max=reach).astype(kind)


def setup_inputs(seed: int = 0) -> dict:
    key_list = jax.random.split(jax.random.key(seed), 7)
    expert_rows = draw_expert_rows(jax.random.fold_in(key_list[6], 71), 0)
    router_input = centred(key_list[1], (TOKENS, DMODEL), 1.0, 6.0, ((0, 32),))
    router_weight = centred(key_list[2], (DMODEL, EXPERTS), DMODEL ** -0.5, 0.09375, (), jnp.float32)
    assign = picks_of(key_list[3], TOKENS, EXPERTS, 2, 4096)
    targets = set_ends(ranked_ids(key_list[4], (TOKENS,), VOCAB, 2), jax.random.fold_in(key_list[4], 3), 0, VOCAB - 1).astype(jnp.int32)
    head = draw_head(jax.random.fold_in(key_list[6], 71), 0)
    return {"expert_rows": expert_rows, "router_input": router_input, "router_weight": router_weight, "assign": assign, "targets": targets, "head": head}


def reference(expert_rows, router_input, router_weight, assign, targets, head):
    inputs = router_input.astype(jnp.float32)
    gate_logits = jnp.dot(inputs, router_weight, precision=lax.Precision.HIGHEST)
    labels = jnp.arange(EXPERTS, dtype=jnp.int32)
    first_hot = (assign[:, 0:1] == labels[None, :]).astype(jnp.float32)
    second_hot = (assign[:, 1:2] == labels[None, :]).astype(jnp.float32)
    differ = first_hot - second_hot
    mix_share = jax.nn.sigmoid(lax.optimization_barrier(jnp.sum(gate_logits * differ, axis=1)))
    mixing = mix_share[:, None] * first_hot + (1.0 - mix_share)[:, None] * second_hot
    block_rows = 512 if TOKENS % 512 == 0 else TOKENS
    quarter = VOCAB // N_EXP
    loss_scale = 1.0 / math.sqrt(TOKENS)
    vocab_ids = jnp.arange(VOCAB, dtype=jnp.int32)

    def one_block(position):
        offset = (position * block_rows).astype(jnp.int32)
        block_experts = lax.dynamic_slice_in_dim(expert_rows, offset, block_rows, 1).astype(jnp.float32)
        weights = lax.dynamic_slice_in_dim(mixing, offset, block_rows, 0)
        wanted = lax.dynamic_slice_in_dim(targets, offset, block_rows, 0)
        mixed_rows = lax.optimization_barrier(jnp.sum(weights.T[:, :, None] * block_experts, axis=0)).astype(jnp.bfloat16)
        logits = jnp.dot(mixed_rows, head, preferred_element_type=jnp.float32)
        row_top = lax.optimization_barrier(jnp.max(logits, axis=1))
        log_total = row_top + jnp.log(lax.optimization_barrier(jnp.sum(jnp.exp(logits - row_top[:, None]), axis=1)))
        target_hit = wanted[:, None] == vocab_ids[None, :]
        tok_loss = log_total - lax.optimization_barrier(jnp.sum(jnp.where(target_hit, logits, 0.0), axis=1))
        slope = (loss_scale * (jnp.exp(logits - log_total[:, None]) - target_hit.astype(jnp.float32))).astype(jnp.bfloat16)
        hidden = jnp.zeros((block_rows, DMODEL), jnp.float32)
        for quart in range(N_EXP):
            partial_value = lax.dot_general(slope[:, quart * quarter:(quart + 1) * quarter], head[:, quart * quarter:(quart + 1) * quarter], (((1,), (1,)), ((), ())), preferred_element_type=jnp.float32)
            hidden = hidden + lax.optimization_barrier(partial_value.astype(jnp.bfloat16)).astype(jnp.float32)
        weight_slope = lax.optimization_barrier(jnp.sum(hidden[None, :, :] * block_experts, axis=2)).T
        return (tok_loss, weight_slope)
    token_loss, weight_slope = lax.map(one_block, jnp.arange(TOKENS // block_rows))
    token_loss = token_loss.reshape(TOKENS)
    weight_slope = weight_slope.reshape(TOKENS, EXPERTS)
    spread = lax.optimization_barrier(jnp.sum(weight_slope * differ, axis=1)) * mix_share * (1.0 - mix_share)
    gate_slope = spread[:, None] * differ
    router_grad = jnp.dot(inputs.T, gate_slope, precision=lax.Precision.HIGHEST)
    mean_loss = jnp.sum(token_loss) / TOKENS
    return (token_loss, router_grad, mean_loss)
```

```python
import functools
import math

import jax
import jax.numpy as jnp
from jax import lax
from jax.experimental import pallas as pl
from jax.experimental.pallas import tpu as pltpu
from jax.sharding import PartitionSpec as P

MESH = pl.DeviceIdType.MESH
F32 = jnp.float32
BF16 = jnp.bfloat16
TILE = 512


def plane(n_tok):
    chips = n_tok // 2
    ny = max(d for d in range(1, math.isqrt(chips) + 1) if chips % d == 0)
    return ny, chips // ny


def kernel(cfg, expert_ref, head_ref, x_ref, wt_ref, assign_ref, tgt_ref,
           loss_ref, grad_ref,
           wide, rows, mixed, drow, tgt, logits, slope, hid, hrecv, stat, part, part_in, chip_in, z_in, both,
           loc_sem, head_s, head_r, core_s, core_r, row_s, row_r, mix_s, mix_r, tgt_s, tgt_r, st_s, st_r,
           hid_s, hid_r, red_s, red_r, chip_s, chip_r, z_s, z_r):
    n_tok, n_exp, vocab, experts, tokens_all = cfg
    ny, nx = plane(n_tok)
    chips = ny * nx
    me, z = lax.axis_index("tok"), lax.axis_index("exp")
    chip, core = me // 2, lax.rem(me, 2)
    cy, cx = chip // nx, lax.rem(chip, nx)
    mate = chip * 2 + (1 - core)
    right_x = (cy * nx + lax.rem(cx + 1, nx)) * 2 + core
    right_y = (lax.rem(cy + 1, ny) * nx + cx) * 2 + core
    own, dim = x_ref.shape
    group = own * n_exp
    block, width = head_ref.shape
    half = block // 2
    tiles = width // TILE

    def slot(ry, rx, rc):
        return (ry * nx + rx) * 2 + rc

    def owner(ry, rx, rc):
        oy, ox = lax.rem(cy - ry + ny, ny), lax.rem(cx - rx + nx, nx)
        return (oy * nx + ox) * 2 + (core if rc == 0 else 1 - core)

    def remote(src, dst, send, recv, tok, exp):
        return pltpu.make_async_remote_copy(src_ref=src, dst_ref=dst, send_sem=send, recv_sem=recv,
                                            device_id=(tok, exp), device_id_type=MESH)

    sends = []

    def go(copy):
        copy.start()
        sends.append(copy)
        return copy

    incoming = {}
    core_in = {}

    def piece(ref, h):
        return ref.at[pl.ds(h * half, half), :]

    def forward(ry, rx, h):
        source = piece(head_ref, h) if (ry, rx) == (0, 0) else piece(wide.at[slot(ry, rx, 0)], h)
        hops = []
        if h == 0:
            if ry == 0 and rx < nx - 1:
                hops.append(("x", ry, rx + 1))
            if ry < ny - 1:
                hops.append(("y", ry + 1, rx))
        else:
            if rx == 0 and ry < ny - 1:
                hops.append(("y", ry + 1, rx))
            if rx < nx - 1:
                hops.append(("x", ry, rx + 1))
        for axis, ty, tx in hops:
            k = slot(ty, tx, 0)
            incoming[ty, tx, h] = go(remote(source, piece(wide.at[k], h), head_s.at[k, h], head_r.at[k, h],
                                            right_x if axis == "x" else right_y, z))
        k = slot(ry, rx, 1)
        core_in[ry, rx, h] = go(remote(source, piece(wide.at[k], h), core_s.at[k, h], core_r.at[k, h], mate, z))

    forward(0, 0, 0)
    forward(0, 0, 1)
    own_head = pltpu.make_async_copy(head_ref, wide.at[0], loc_sem.at[0])
    own_head.start()

    row_in, tgt_in = [], []
    mine = pl.ds(pl.multiple_of(z * own, own), own)
    for k in range(1, n_exp):
        peer = lax.rem(z + k, n_exp)
        theirs = pl.ds(pl.multiple_of(peer * own, own), own)
        row_in.append(go(remote(expert_ref.at[0, theirs, :], rows.at[z], row_s.at[k], row_r.at[k], me, peer)))
        tgt_in.append(go(remote(tgt_ref, tgt.at[mine, :], tgt_s.at[k], tgt_r.at[k], me, peer)))
    own_rows = pltpu.make_async_copy(expert_ref.at[0, mine, :], rows.at[z], loc_sem.at[1])
    own_rows.start()
    tgt[mine, :] = tgt_ref[...]

    def clear(i, _):
        logits[:, pl.ds(pl.multiple_of(i * TILE, TILE), TILE)] = jnp.zeros((group, TILE), F32)
        return 0

    lax.fori_loop(0, tiles, clear, 0)

    chosen = assign_ref[...]
    first = [(chosen[:, 0:1] == e).astype(F32) for e in range(experts)]
    second = [(chosen[:, 1:2] == e).astype(F32) for e in range(experts)]
    differ = [f - s for f, s in zip(first, second)]
    cols = TILE
    steps = dim // cols

    def gate_step(i, acc):
        at = pl.ds(pl.multiple_of(i * cols, cols), cols)
        x = x_ref[:, at].astype(F32)
        return tuple(a + jnp.sum(x * wt_ref[e:e + 1, at], axis=1, keepdims=True) for e, a in enumerate(acc))

    gates = lax.fori_loop(0, steps, gate_step, tuple(jnp.zeros((own, 1), F32) for _ in range(experts)))
    share = jax.nn.sigmoid(sum(g * d for g, d in zip(gates, differ)))
    mixing = [share * f + (1.0 - share) * s for f, s in zip(first, second)]

    own_rows.wait()
    for copy in row_in:
        copy.wait_recv()

    def mix_step(i, _):
        at = pl.ds(pl.multiple_of(i * cols, cols), cols)
        total = jnp.zeros((own, cols), F32)
        apart = jnp.zeros((own, cols), F32)
        for e in range(experts):
            r = rows[e, :, at].astype(F32)
            total = total + mixing[e] * r
            apart = apart + differ[e] * r
        mixed[mine, at] = total.astype(BF16)
        drow[:, at] = apart
        return 0

    lax.fori_loop(0, steps, mix_step, 0)
    mix_in = []
    for k in range(1, n_exp):
        peer = lax.rem(z + k, n_exp)
        mix_in.append(go(remote(mixed.at[mine, :], mixed.at[mine, :], mix_s.at[k], mix_r.at[k], me, peer)))
    for copy in mix_in + tgt_in:
        copy.wait_recv()

    def add_block(ry, rx, rc):
        k = slot(ry, rx, rc)
        left = mixed[:, pl.ds(pl.multiple_of(owner(ry, rx, rc) * block, block), block)]

        def step(i, _):
            at = pl.ds(pl.multiple_of(i * TILE, TILE), TILE)
            logits[:, at] += jnp.dot(left, wide[k, :, at], preferred_element_type=F32)
            return 0

        lax.fori_loop(0, tiles, step, 0)

    def add_mate(ry, rx):
        for h in range(2):
            core_in[ry, rx, h].wait_recv()
        add_block(ry, rx, 1)

    own_head.wait()
    add_block(0, 0, 0)
    add_mate(0, 0)
    order = sorted(
        ((ry, rx, h) for ry in range(ny) for rx in range(nx) for h in range(2) if ry + rx > 0),
        key=lambda p: (p[0] + p[1], p[0] if p[2] == 0 else p[1], p[2]),
    )
    here, ready = {}, []
    for ry, rx, h in order:
        incoming[ry, rx, h].wait_recv()
        forward(ry, rx, h)
        here[ry, rx] = here.get((ry, rx), 0) + 1
        if here[ry, rx] == 2:
            for pair in ready:
                add_mate(*pair)
            ready = [(ry, rx)]
            add_block(ry, rx, 0)
    for pair in ready:
        add_mate(*pair)

    lane = lax.broadcasted_iota(jnp.int32, (group, TILE), 1)
    low = jnp.float32(-3.0e38)

    def top_step(i, m):
        at = pl.ds(pl.multiple_of(i * TILE, TILE), TILE)
        v = jnp.where(lane + i * TILE < vocab, logits[:, at], low)
        return jnp.maximum(m, jnp.max(v, axis=1, keepdims=True))

    top = lax.fori_loop(0, tiles, top_step, jnp.full((group, 1), low, F32))
    wanted = tgt[:, 0:1] - z * vocab

    def hit_of(i):
        col = lane + i * TILE
        return jnp.logical_and(col == wanted, col < vocab)

    def sum_step(i, carry):
        s, p = carry
        at = pl.ds(pl.multiple_of(i * TILE, TILE), TILE)
        v = logits[:, at]
        e = jnp.where(lane + i * TILE < vocab, jnp.exp(v - top), 0.0)
        p = p + jnp.sum(jnp.where(hit_of(i), v, 0.0), axis=1, keepdims=True)
        logits[:, at] = e
        return s + jnp.sum(e, axis=1, keepdims=True), p

    zero = jnp.zeros((group, 1), F32)
    total, picked = lax.fori_loop(0, tiles, sum_step, (zero, zero))
    narrow = lax.broadcasted_iota(jnp.int32, (group, 128), 1)
    packed = jnp.where(narrow == 0, top, jnp.where(narrow == 1, total, jnp.where(narrow == 2, picked, 0.0)))
    stat[z] = packed.T[0:8, :]
    st_in = []
    for k in range(1, n_exp):
        peer = lax.rem(z + k, n_exp)
        st_in.append(go(remote(stat.at[z], stat.at[z], st_s.at[k], st_r.at[k], me, peer)))
    for copy in st_in:
        copy.wait_recv()
    stats = [stat[q] for q in range(n_exp)]
    row_top = functools.reduce(jnp.maximum, [s[0:1, :] for s in stats])
    exp_total = sum(s[1:2, :] * jnp.exp(s[0:1, :] - row_top) for s in stats)
    log_total = row_top + jnp.log(exp_total)
    loss = log_total - sum(s[2:3, :] for s in stats)
    loss_ref[...] = loss
    column = jnp.broadcast_to(log_total, (128, group)).T[:, 0:1]
    factor = jnp.exp(top - column)
    scale = 1.0 / math.sqrt(tokens_all)

    def slope_step(i, _):
        at = pl.ds(pl.multiple_of(i * TILE, TILE), TILE)
        slope[:, at] = (scale * (logits[:, at] * factor - hit_of(i).astype(F32))).astype(BF16)
        return 0

    lax.fori_loop(0, tiles, slope_step, 0)

    def hid_copy(k, j):
        peer = lax.rem(z + j, n_exp)
        return remote(hid.at[k, peer], hrecv.at[k, j], hid_s.at[k, j], hid_r.at[k, j], me, peer)

    def back_step(k, _):
        out = lax.dot_general(slope[...], wide[k], (((1,), (1,)), ((), ())), preferred_element_type=F32)
        hid[k] = out.astype(BF16).reshape(n_exp, own, block)
        for j in range(1, n_exp):
            hid_copy(k, j).start()
        return 0

    lax.fori_loop(0, n_tok, back_step, 0)

    acc = jnp.zeros((own, 1), F32)
    for ry in range(ny):
        for rx in range(nx):
            for rc in range(2):
                k = slot(ry, rx, rc)
                hidden = hid[k, z].astype(F32)
                for j in range(1, n_exp):
                    hid_copy(k, j).wait_recv()
                    hidden = hidden + hrecv[k, j].astype(F32)
                at = pl.ds(pl.multiple_of(owner(ry, rx, rc) * block, block), block)
                acc = acc + jnp.sum(hidden * drow[:, at], axis=1, keepdims=True)
    spread = acc * share * (1.0 - share)
    weights = [spread * d for d in differ]

    quarter = dim // 4
    loss_share = jnp.sum(loss, axis=1, keepdims=True) * (1.0 / n_exp)
    for c in range(2):
        for q in range(2):
            x = x_ref[:, (c * 2 + q) * quarter:(c * 2 + q + 1) * quarter].astype(F32)
            for e in range(experts):
                part[c, q * experts + e:q * experts + e + 1, 0:quarter] = jnp.sum(weights[e] * x, axis=0, keepdims=True)
        part[c, :, quarter:quarter + 128] = jnp.broadcast_to(loss_share, (2 * experts, 128))
    trade = go(remote(part.at[1 - core], part_in, red_s.at[0], red_r.at[0], mate, z))
    trade.wait_recv()
    chip_in[chip] = part[core] + part_in[...]
    copies = []
    for k in range(1, chips):
        there = lax.rem(chip + k, chips)
        copies.append(go(remote(chip_in.at[chip], chip_in.at[chip], chip_s.at[k], chip_r.at[k], there * 2 + core, z)))
    for copy in copies:
        copy.wait_recv()
    z_in[z] = sum(chip_in[k] for k in range(chips))
    copies = []
    for k in range(1, n_exp):
        peer = lax.rem(z + k, n_exp)
        copies.append(go(remote(z_in.at[z], z_in.at[z], z_s.at[k], z_r.at[k], me, peer)))
    for copy in copies:
        copy.wait_recv()
    both[core] = sum(z_in[k] for k in range(n_exp))
    trade = go(remote(both.at[core], both.at[core], red_s.at[1], red_r.at[1], mate, z))
    trade.wait_recv()
    grad_ref[...] = both[...]

    for copy in sends:
        copy.wait_send()

    def drain(k, _):
        for j in range(1, n_exp):
            hid_copy(k, j).wait_send()
        return 0

    lax.fori_loop(0, n_tok, drain, 0)


def shards(n_tok, n_exp, expert_rows, router_input, router_weight, assign, targets, head):
    experts = router_weight.shape[1]
    own, dim = router_input.shape
    group = own * n_exp
    tokens_all = own * n_tok * n_exp
    block, vocab = head.shape
    width = -(-vocab // TILE) * TILE
    head = jnp.pad(head, ((0, 0), (0, width - vocab)))
    wide_targets = jnp.broadcast_to(targets[:, None], (own, 128))
    quarter = dim // 4
    packed = (2 * experts, quarter + 128)
    vmem = pl.BlockSpec(memory_space=pltpu.VMEM)
    hbm = pl.BlockSpec(memory_space=pl.ANY)
    dma = pltpu.SemaphoreType.DMA
    chips = n_tok // 2
    loss, grad = pl.pallas_call(
        functools.partial(kernel, (n_tok, n_exp, vocab, experts, tokens_all)),
        out_shape=(jax.ShapeDtypeStruct((1, group), F32), jax.ShapeDtypeStruct((2,) + packed, F32)),
        in_specs=[hbm, hbm, vmem, vmem, vmem, vmem],
        out_specs=(vmem, vmem),
        scratch_shapes=[
            pltpu.VMEM((n_tok, block, width), BF16),
            pltpu.VMEM((experts, own, dim), BF16),
            pltpu.VMEM((group, dim), BF16),
            pltpu.VMEM((own, dim), F32),
            pltpu.VMEM((group, 128), jnp.int32),
            pltpu.VMEM((group, width), F32),
            pltpu.VMEM((group, width), BF16),
            pltpu.VMEM((n_tok, n_exp, own, block), BF16),
            pltpu.VMEM((n_tok, n_exp, own, block), BF16),
            pltpu.VMEM((n_exp, 8, group), F32),
            pltpu.VMEM((2,) + packed, F32),
            pltpu.VMEM(packed, F32),
            pltpu.VMEM((chips,) + packed, F32),
            pltpu.VMEM((n_exp,) + packed, F32),
            pltpu.VMEM((2,) + packed, F32),
            dma((2,)),
            dma((n_tok, 2)), dma((n_tok, 2)), dma((n_tok, 2)), dma((n_tok, 2)),
            dma((n_exp,)), dma((n_exp,)), dma((n_exp,)), dma((n_exp,)),
            dma((n_exp,)), dma((n_exp,)), dma((n_exp,)), dma((n_exp,)),
            dma((n_tok, n_exp)), dma((n_tok, n_exp)),
            dma((2,)), dma((2,)),
            dma((chips,)), dma((chips,)), dma((n_exp,)), dma((n_exp,)),
        ],
        compiler_params=pltpu.CompilerParams(has_side_effects=True, vmem_limit_bytes=62 * 1024 * 1024),
        name="router_step",
    )(expert_rows, head, router_input, router_weight.T, assign, wide_targets)
    own_loss = lax.dynamic_slice_in_dim(loss[0], lax.axis_index("exp") * own, own, 0)
    router_sum = grad[:, :, :quarter].reshape(2, 2, experts, quarter).transpose(0, 1, 3, 2).reshape(dim, experts)
    mean_loss = grad[0, 0, quarter] / tokens_all
    return (own_loss, router_sum, mean_loss)


def solution(mesh):
    in_specs = (
        P("exp", "tok", None),
        P(("tok", "exp"), None),
        P(),
        P(("tok", "exp"), None),
        P(("tok", "exp")),
        P("tok", "exp"),
    )
    out_specs = (P(("tok", "exp")), P(), P())
    body = functools.partial(shards, mesh.shape["tok"], mesh.shape["exp"])
    return jax.shard_map(body, mesh=mesh, in_specs=in_specs, out_specs=out_specs, check_vma=False)
```

```python
import functools
import math

import jax
import jax.numpy as jnp
from jax import lax
from jax.experimental import pallas as pl
from jax.experimental.pallas import tpu as pltpu
from jax.sharding import PartitionSpec as P

MESH = pl.DeviceIdType.MESH
F32 = jnp.float32
BF16 = jnp.bfloat16
TILE = 512


def plane(n_tok):
    chips = n_tok // 2
    ny = max(d for d in range(1, math.isqrt(chips) + 1) if chips % d == 0)
    return ny, chips // ny


def kernel(cfg, expert_ref, head_ref, x_ref, wt_ref, assign_ref, tgt_ref,
           loss_ref, grad_ref,
           wide, rows, mixed, drow, tgt, logits, slope, hid, hrecv, relay, stat, part, part_in, chip_in, z_in, both,
           loc_sem, head_s, head_r, core_s, core_r, row_s, row_r, mix_s, mix_r, tgt_s, tgt_r, st_s, st_r,
           hid_s, hid_r, red_s, red_r, chip_s, chip_r, z_s, z_r):
    n_tok, n_exp, vocab, experts, tokens_all = cfg
    ny, nx = plane(n_tok)
    chips = ny * nx
    me, z = lax.axis_index("tok"), lax.axis_index("exp")
    chip, core = me // 2, lax.rem(me, 2)
    cy, cx = chip // nx, lax.rem(chip, nx)
    mate = chip * 2 + (1 - core)
    right_x = (cy * nx + lax.rem(cx + 1, nx)) * 2 + core
    right_y = (lax.rem(cy + 1, ny) * nx + cx) * 2 + core
    own, dim = x_ref.shape
    group = own * n_exp
    block = head_ref.shape[1]
    width = wide.shape[1]
    split = vocab // 32 * 16
    tiles = width // TILE

    def slot(ry, rx, rc):
        return (ry * nx + rx) * 2 + rc

    def owner(ry, rx, rc):
        oy, ox = lax.rem(cy - ry + ny, ny), lax.rem(cx - rx + nx, nx)
        return (oy * nx + ox) * 2 + (core if rc == 0 else 1 - core)

    def remote(src, dst, send, recv, tok, exp):
        return pltpu.make_async_remote_copy(src_ref=src, dst_ref=dst, send_sem=send, recv_sem=recv,
                                            device_id=(tok, exp), device_id_type=MESH)

    sends = []

    def go(copy):
        copy.start()
        sends.append(copy)
        return copy

    incoming = {}
    core_in = {}

    def piece(ref, h):
        return ref.at[pl.ds(split, vocab - split), :] if h else ref.at[pl.ds(0, split), :]

    def forward(ry, rx, h):
        source = piece(head_ref, h) if (ry, rx) == (0, 0) else piece(wide.at[slot(ry, rx, 0)], h)
        hops = []
        if h == 0:
            if ry == 0 and rx < nx - 1:
                hops.append(("x", ry, rx + 1))
            if ry < ny - 1:
                hops.append(("y", ry + 1, rx))
        else:
            if rx == 0 and ry < ny - 1:
                hops.append(("y", ry + 1, rx))
            if rx < nx - 1:
                hops.append(("x", ry, rx + 1))
        for axis, ty, tx in hops:
            k = slot(ty, tx, 0)
            incoming[ty, tx, h] = go(remote(source, piece(wide.at[k], h), head_s.at[k, h], head_r.at[k, h],
                                            right_x if axis == "x" else right_y, z))
        k = slot(ry, rx, 1)
        core_in[ry, rx, h] = go(remote(source, piece(wide.at[k], h), core_s.at[k, h], core_r.at[k, h], mate, z))

    forward(0, 0, 0)
    forward(0, 0, 1)
    own_head = pltpu.make_async_copy(head_ref, wide.at[0, pl.ds(0, vocab), :], loc_sem.at[0])
    own_head.start()

    row_in, tgt_in = [], []
    mine = pl.ds(pl.multiple_of(z * own, own), own)
    for k in range(1, n_exp):
        peer = lax.rem(z + k, n_exp)
        theirs = pl.ds(pl.multiple_of(peer * own, own), own)
        row_in.append(go(remote(expert_ref.at[0, theirs, :], rows.at[z], row_s.at[k], row_r.at[k], me, peer)))
        tgt_in.append(go(remote(tgt_ref, tgt.at[mine, :], tgt_s.at[k], tgt_r.at[k], me, peer)))
    own_rows = pltpu.make_async_copy(expert_ref.at[0, mine, :], rows.at[z], loc_sem.at[1])
    own_rows.start()
    tgt[mine, :] = tgt_ref[...]

    def clear(i, _):
        logits[:, pl.ds(pl.multiple_of(i * TILE, TILE), TILE)] = jnp.zeros((group, TILE), F32)
        return 0

    lax.fori_loop(0, tiles, clear, 0)
    if width > vocab:
        for k in range(n_tok):
            wide[k, vocab:width, :] = jnp.zeros((width - vocab, block), BF16)

    chosen = assign_ref[...]
    first = [(chosen[:, 0:1] == e).astype(F32) for e in range(experts)]
    second = [(chosen[:, 1:2] == e).astype(F32) for e in range(experts)]
    differ = [f - s for f, s in zip(first, second)]
    cols = TILE
    steps = dim // cols

    def gate_step(i, acc):
        at = pl.ds(pl.multiple_of(i * cols, cols), cols)
        x = x_ref[:, at].astype(F32)
        return tuple(a + jnp.sum(x * wt_ref[e:e + 1, at], axis=1, keepdims=True) for e, a in enumerate(acc))

    gates = lax.fori_loop(0, steps, gate_step, tuple(jnp.zeros((own, 1), F32) for _ in range(experts)))
    share = jax.nn.sigmoid(sum(g * d for g, d in zip(gates, differ)))
    mixing = [share * f + (1.0 - share) * s for f, s in zip(first, second)]

    own_rows.wait()
    for copy in row_in:
        copy.wait_recv()

    def mix_step(i, _):
        at = pl.ds(pl.multiple_of(i * cols, cols), cols)
        total = jnp.zeros((own, cols), F32)
        apart = jnp.zeros((own, cols), F32)
        for e in range(experts):
            r = rows[e, :, at].astype(F32)
            total = total + mixing[e] * r
            apart = apart + differ[e] * r
        mixed[mine, at] = total.astype(BF16)
        drow[:, at] = apart
        return 0

    lax.fori_loop(0, steps, mix_step, 0)
    mix_in = []
    for k in range(1, n_exp):
        peer = lax.rem(z + k, n_exp)
        mix_in.append(go(remote(mixed.at[mine, :], mixed.at[mine, :], mix_s.at[k], mix_r.at[k], me, peer)))
    for copy in mix_in + tgt_in:
        copy.wait_recv()

    def add_block(ry, rx, rc):
        k = slot(ry, rx, rc)
        left = mixed[:, pl.ds(pl.multiple_of(owner(ry, rx, rc) * block, block), block)]

        def step(i, _):
            at = pl.ds(pl.multiple_of(i * TILE, TILE), TILE)
            logits[:, at] += lax.dot_general(
                left, wide[k, at, :], (((1,), (1,)), ((), ())), preferred_element_type=F32)
            return 0

        lax.fori_loop(0, tiles, step, 0)

    def add_mate(ry, rx):
        for h in range(2):
            core_in[ry, rx, h].wait_recv()
        add_block(ry, rx, 1)

    own_head.wait()
    add_block(0, 0, 0)
    add_mate(0, 0)
    order = sorted(
        ((ry, rx, h) for ry in range(ny) for rx in range(nx) for h in range(2) if ry + rx > 0),
        key=lambda p: (p[0] + p[1], p[0] if p[2] == 0 else p[1], p[2]),
    )
    here, ready = {}, []
    for ry, rx, h in order:
        incoming[ry, rx, h].wait_recv()
        forward(ry, rx, h)
        here[ry, rx] = here.get((ry, rx), 0) + 1
        if here[ry, rx] == 2:
            for pair in ready:
                add_mate(*pair)
            ready = [(ry, rx)]
            add_block(ry, rx, 0)
    for pair in ready:
        add_mate(*pair)

    lane = lax.broadcasted_iota(jnp.int32, (group, TILE), 1)
    low = jnp.float32(-3.0e38)

    def top_step(i, m):
        at = pl.ds(pl.multiple_of(i * TILE, TILE), TILE)
        v = jnp.where(lane + i * TILE < vocab, logits[:, at], low)
        return jnp.maximum(m, jnp.max(v, axis=1, keepdims=True))

    top = lax.fori_loop(0, tiles, top_step, jnp.full((group, 1), low, F32))
    wanted = tgt[:, 0:1] - z * vocab

    def hit_of(i):
        col = lane + i * TILE
        return jnp.logical_and(col == wanted, col < vocab)

    def sum_step(i, carry):
        s, p = carry
        at = pl.ds(pl.multiple_of(i * TILE, TILE), TILE)
        v = logits[:, at]
        e = jnp.where(lane + i * TILE < vocab, jnp.exp(v - top), 0.0)
        p = p + jnp.sum(jnp.where(hit_of(i), v, 0.0), axis=1, keepdims=True)
        logits[:, at] = e
        return s + jnp.sum(e, axis=1, keepdims=True), p

    zero = jnp.zeros((group, 1), F32)
    total, picked = lax.fori_loop(0, tiles, sum_step, (zero, zero))
    narrow = lax.broadcasted_iota(jnp.int32, (group, 128), 1)
    packed = jnp.where(narrow == 0, top, jnp.where(narrow == 1, total, jnp.where(narrow == 2, picked, 0.0)))
    stat[z] = packed.T[0:8, :]
    st_in = []
    for k in range(1, n_exp):
        peer = lax.rem(z + k, n_exp)
        st_in.append(go(remote(stat.at[z], stat.at[z], st_s.at[k], st_r.at[k], me, peer)))
    for copy in st_in:
        copy.wait_recv()
    stats = [stat[q] for q in range(n_exp)]
    row_top = functools.reduce(jnp.maximum, [s[0:1, :] for s in stats])
    exp_total = sum(s[1:2, :] * jnp.exp(s[0:1, :] - row_top) for s in stats)
    log_total = row_top + jnp.log(exp_total)
    loss = log_total - sum(s[2:3, :] for s in stats)
    loss_ref[...] = loss
    column = jnp.broadcast_to(log_total, (128, group)).T[:, 0:1]
    factor = jnp.exp(top - column)
    scale = 1.0 / math.sqrt(tokens_all)

    def slope_step(i, _):
        at = pl.ds(pl.multiple_of(i * TILE, TILE), TILE)
        slope[:, at] = (scale * (logits[:, at] * factor - hit_of(i).astype(F32))).astype(BF16)
        return 0

    lax.fori_loop(0, tiles, slope_step, 0)

    def hid_copy(k, j):
        peer = lax.rem(z + j, n_exp)
        return remote(hid.at[k, peer], hrecv.at[k, j], hid_s.at[k, j], hid_r.at[k, j], me, peer)

    ringed = n_exp == 4
    near = (1, 3) if ringed else tuple(range(1, n_exp))
    ahead, behind, far = lax.rem(z + 1, n_exp), lax.rem(z + n_exp - 1, n_exp), lax.rem(z + 2, n_exp)
    low_half = own // 2

    def relay_copy(k, side):
        return remote(hid.at[k, far, pl.ds(side * low_half, low_half), :], relay.at[k, side],
                      hid_s.at[k, 2 * side], hid_r.at[k, 2 * side], me, behind if side else ahead)

    def pass_on(k):
        for side, target in enumerate((ahead, behind)):
            relay_copy(k, side).wait_recv()
            at = pl.ds(side * low_half, low_half)
            joined = hid[k, target, at, :].astype(F32) + relay[k, side].astype(F32)
            hid[k, target, at, :] = joined.astype(BF16)
        for j in near:
            hid_copy(k, j).start()

    def back_step(k, _):
        out = jnp.dot(slope[...], wide[k], preferred_element_type=F32)
        hid[k] = out.astype(BF16).reshape(n_exp, own, block)
        if ringed:
            for side in range(2):
                relay_copy(k, side).start()
            pl.when(k > 0)(lambda: pass_on(k - 1))
        else:
            for j in near:
                hid_copy(k, j).start()
        return 0

    lax.fori_loop(0, n_tok, back_step, 0)
    if ringed:
        pass_on(n_tok - 1)

    acc = jnp.zeros((own, 1), F32)
    for ry in range(ny):
        for rx in range(nx):
            for rc in range(2):
                k = slot(ry, rx, rc)
                hidden = hid[k, z].astype(F32)
                for j in near:
                    hid_copy(k, j).wait_recv()
                    hidden = hidden + hrecv[k, j].astype(F32)
                at = pl.ds(pl.multiple_of(owner(ry, rx, rc) * block, block), block)
                acc = acc + jnp.sum(hidden * drow[:, at], axis=1, keepdims=True)
    spread = acc * share * (1.0 - share)
    weights = [spread * d for d in differ]

    quarter = dim // 4
    loss_share = jnp.sum(loss, axis=1, keepdims=True) * (1.0 / n_exp)
    for c in range(2):
        for q in range(2):
            x = x_ref[:, (c * 2 + q) * quarter:(c * 2 + q + 1) * quarter].astype(F32)
            for e in range(experts):
                part[c, q * experts + e:q * experts + e + 1, 0:quarter] = jnp.sum(weights[e] * x, axis=0, keepdims=True)
        part[c, :, quarter:quarter + 128] = jnp.broadcast_to(loss_share, (2 * experts, 128))
    trade = go(remote(part.at[1 - core], part_in, red_s.at[0], red_r.at[0], mate, z))
    trade.wait_recv()
    chip_in[chip] = part[core] + part_in[...]
    copies = []
    for k in range(1, chips):
        there = lax.rem(chip + k, chips)
        copies.append(go(remote(chip_in.at[chip], chip_in.at[chip], chip_s.at[k], chip_r.at[k], there * 2 + core, z)))
    for copy in copies:
        copy.wait_recv()
    z_in[z] = sum(chip_in[k] for k in range(chips))
    copies = []
    for k in range(1, n_exp):
        peer = lax.rem(z + k, n_exp)
        copies.append(go(remote(z_in.at[z], z_in.at[z], z_s.at[k], z_r.at[k], me, peer)))
    for copy in copies:
        copy.wait_recv()
    both[core] = sum(z_in[k] for k in range(n_exp))
    trade = go(remote(both.at[core], both.at[core], red_s.at[1], red_r.at[1], mate, z))
    trade.wait_recv()
    grad_ref[...] = both[...]

    for copy in sends:
        copy.wait_send()

    def drain(k, _):
        for j in near:
            hid_copy(k, j).wait_send()
        if ringed:
            for side in range(2):
                relay_copy(k, side).wait_send()
        return 0

    lax.fori_loop(0, n_tok, drain, 0)


def shards(n_tok, n_exp, expert_rows, router_input, router_weight, assign, targets, head):
    experts = router_weight.shape[1]
    own, dim = router_input.shape
    group = own * n_exp
    tokens_all = own * n_tok * n_exp
    block, vocab = head.shape
    width = -(-vocab // TILE) * TILE
    wide_targets = jnp.broadcast_to(targets[:, None], (own, 128))
    quarter = dim // 4
    packed = (2 * experts, quarter + 128)
    vmem = pl.BlockSpec(memory_space=pltpu.VMEM)
    hbm = pl.BlockSpec(memory_space=pl.ANY)
    dma = pltpu.SemaphoreType.DMA
    chips = n_tok // 2
    loss, grad = pl.pallas_call(
        functools.partial(kernel, (n_tok, n_exp, vocab, experts, tokens_all)),
        out_shape=(jax.ShapeDtypeStruct((1, group), F32), jax.ShapeDtypeStruct((2,) + packed, F32)),
        in_specs=[hbm, hbm, vmem, vmem, vmem, vmem],
        out_specs=(vmem, vmem),
        scratch_shapes=[
            pltpu.VMEM((n_tok, width, block), BF16),
            pltpu.VMEM((experts, own, dim), BF16),
            pltpu.VMEM((group, dim), BF16),
            pltpu.VMEM((own, dim), F32),
            pltpu.VMEM((group, 128), jnp.int32),
            pltpu.VMEM((group, width), F32),
            pltpu.VMEM((group, width), BF16),
            pltpu.VMEM((n_tok, n_exp, own, block), BF16),
            pltpu.VMEM((n_tok, n_exp, own, block), BF16),
            pltpu.VMEM((n_tok, 2, own // 2, block), BF16),
            pltpu.VMEM((n_exp, 8, group), F32),
            pltpu.VMEM((2,) + packed, F32),
            pltpu.VMEM(packed, F32),
            pltpu.VMEM((chips,) + packed, F32),
            pltpu.VMEM((n_exp,) + packed, F32),
            pltpu.VMEM((2,) + packed, F32),
            dma((2,)),
            dma((n_tok, 2)), dma((n_tok, 2)), dma((n_tok, 2)), dma((n_tok, 2)),
            dma((n_exp,)), dma((n_exp,)), dma((n_exp,)), dma((n_exp,)),
            dma((n_exp,)), dma((n_exp,)), dma((n_exp,)), dma((n_exp,)),
            dma((n_tok, n_exp)), dma((n_tok, n_exp)),
            dma((2,)), dma((2,)),
            dma((chips,)), dma((chips,)), dma((n_exp,)), dma((n_exp,)),
        ],
        compiler_params=pltpu.CompilerParams(has_side_effects=True, vmem_limit_bytes=62 * 1024 * 1024),
        name="router_step",
    )(expert_rows, head.T, router_input, router_weight.T, assign, wide_targets)
    own_loss = lax.dynamic_slice_in_dim(loss[0], lax.axis_index("exp") * own, own, 0)
    router_sum = grad[:, :, :quarter].reshape(2, 2, experts, quarter).transpose(0, 1, 3, 2).reshape(dim, experts)
    mean_loss = grad[0, 0, quarter] / tokens_all
    return (own_loss, router_sum, mean_loss)


def solution(mesh):
    in_specs = (
        P("exp", "tok", None),
        P(("tok", "exp"), None),
        P(),
        P(("tok", "exp"), None),
        P(("tok", "exp")),
        P("tok", "exp"),
    )
    out_specs = (P(("tok", "exp")), P(), P())
    body = functools.partial(shards, mesh.shape["tok"], mesh.shape["exp"])
    return jax.shard_map(body, mesh=mesh, in_specs=in_specs, out_specs=out_specs, check_vma=False)
```
